32 devices in a mesh: groups: 2 (over x), freq: 8 (over z, y), gvec: 2 (over core).
Axes of the slice: x: 2, y: 2, z: 4, core: 2. Of those that a mesh axis runs over, the one named last changes fastest.
Arguments:
- screened: bfloat16 [16, 3072, 3072], P(('groups', 'freq'), 'gvec'), parts along dimension 0, may hold values from -0.109375 to 0.109375
- densities: bfloat16 [6144, 512], P(('groups', 'gvec'), 'freq'), parts along dimension 0, may hold values from -0.8046875 to 0.8046875
- pair_order: int32 [512], replicated, may hold values from 0 to 511, each once
- quad_index: int32 [4, 8], replicated, may hold values from 0 to 63
- quad_table: float32 [64], replicated, may hold values from 0.05 to 0.5
Outputs:
- kernel_out: float32 [8, 512, 512], P('groups', 'freq', 'gvec'), parts along dimension 0
The draws below stay inside these ranges and needn't reach their ends.
There are 2 independent parts, one for each index of `groups`. The reference program is written for one: setup_inputs(seed, part) draws one part's arguments, and reference() takes and returns one part's arrays. A program takes and returns all parts, laid end to end along the dimension named above; an argument that names none is the same for every part. Nothing has to cross between parts.
All inputs are finite; a program needn't handle non-finite values.
Results may differ from the reference program's by a relative error of at most 0.0029.
Values may be sent and summed in bfloat16 or wider, within the bound.
A program may use at most 64 MiB of HBM per device.

```python
import math
import jax
import jax.numpy as jnp
from jax import lax

GVECS = 3072
PAIRS = 512
ENERGIES = 4
QUAD_ROWS = 64
FREQS = 8


def place_ends(values, key, least, top_value):
    longest = values.shape.index(max(values.shape))
    spots = []
    for shift in (0, 1):
        where = [jax.random.randint(jax.random.fold_in(key, axis), (), 0, length) for axis, length in enumerate(values.shape)]
        where[longest] = (where[longest] + shift) % values.shape[longest]
        spots.append(tuple(where))
    return values.at[spots[0]].set(least).at[spots[1]].set(top_value)


def block_scale(stream_key, extent, shards, low, largest):
    loudness, own = 1.0, jax.random.fold_in(stream_key, 6)
    for dim, blocks in shards:
        steps = jnp.exp(jax.random.uniform(jax.random.fold_in(own, dim), (blocks,), jnp.float32, low / len(shards), largest / len(shards)))
        loudness = loudness * jnp.repeat(steps, extent[dim] // blocks).reshape([-1 if axis == dim else 1 for axis in range(len(extent))])
    return loudness


def normal_values(own_key, extent, spread, reach, cuts=(), kind=jnp.bfloat16):
    entries = spread * jax.random.normal(own_key, extent, jnp.float32)
    if cuts:
        entries = entries * block_scale(own_key, extent, cuts, -0.22, 0.18)
    return jnp.clip(entries, -reach, reach).astype(kind)


def setup_inputs(seed: int = 0, part: int = 0) -> dict:
    key_list = jax.random.split(jax.random.key(seed), 6)
    part_splits = jax.random.split(jax.random.fold_in(key_list[5], part), 6)
    screened = normal_values(part_splits[0], (FREQS, GVECS, GVECS), GVECS ** -0.5, 0.109375, ((0, 8), (1, 2)))
    densities = normal_values(part_splits[1], (GVECS, PAIRS), (GVECS ** -0.25), 0.8046875, ((0, 2), (1, 8)))
    pair_order = jax.random.permutation(key_list[2], PAIRS).astype(jnp.int32)
    quad_index = place_ends(jax.random.randint(key_list[3], (ENERGIES, FREQS), 0, QUAD_ROWS), jax.random.fold_in(key_list[3], 1), 0, QUAD_ROWS - 1).astype(jnp.int32)
    quad_table = jnp.clip(jnp.exp(jax.random.uniform(key_list[4], (QUAD_ROWS,), jnp.float32, math.log(0.05), math.log(0.5))), 0.05, 0.5)
    return {"screened": screened, "densities": densities, "pair_order": pair_order, "quad_index": quad_index, "quad_table": quad_table}


def reference(screened, densities, pair_order, quad_index, quad_table):
    ordered = jnp.take(densities, pair_order, axis=1)
    weights = quad_table[quad_index]

    def advance(running, inputs):
        screen_now, weight_now = inputs
        product = jnp.dot(screen_now, ordered, preferred_element_type=jnp.float32).astype(jnp.bfloat16)
        kernel = jnp.dot(ordered.T, product, preferred_element_type=jnp.float32)
        return running + weight_now[:, None, None] * kernel, None

    start_value = jnp.zeros((ENERGIES, PAIRS, PAIRS), jnp.float32)
    running, unused = lax.scan(advance, start_value, (screened, weights.T))
    return running
```

```python
import functools

import jax
import jax.numpy as jnp
from jax import lax
from jax.experimental import pallas as pl
from jax.experimental.pallas import tpu as pltpu
from jax.sharding import PartitionSpec as P

MESH = pl.DeviceIdType.MESH
F32 = jnp.float32
BF16 = jnp.bfloat16
NT = (((1,), (1,)), ((), ()))


def kernel(
    n, chunks, screened, dens, order, quad_index, quad_table, out,
    w_buf, x_buf, e_buf, acc, p_buf, perm, k_send, k_peer, k_own, k_red, rows_in,
    w_sem, ring_send, ring_recv, pair_send, pair_recv, half_send, half_recv, out_send, out_recv,
):
    rows, per = dens.shape
    pairs = n * per
    half = pairs // 2
    mid = n // 2
    width = rows // chunks
    me = lax.axis_index("freq")
    core = lax.axis_index("gvec")
    peer = 1 - core

    def index_at(position):
        fold = position // mid
        return (1 - fold) * (2 * position) + fold * (2 * (n - 1 - position) + 1)

    odd = me % 2
    place = (1 - odd) * (me // 2) + odd * (n - 1 - me // 2)
    right = index_at((place + 1) % n)
    left = index_at((place + n - 1) % n)

    barrier = pltpu.get_barrier_semaphore()
    pl.semaphore_signal(barrier, inc=1, device_id={"freq": left}, device_id_type=MESH)
    pl.semaphore_signal(barrier, inc=1, device_id={"freq": right}, device_id_type=MESH)
    pl.semaphore_signal(barrier, inc=1, device_id={"gvec": peer}, device_id_type=MESH)

    def w_copy(c, h):
        columns = pl.ds(h * rows + c * width, width)
        return pltpu.make_async_copy(
            screened.at[0, :, columns], w_buf.at[c, h], w_sem.at[c, h]
        )

    for c in range(chunks):
        for h in range(2):
            w_copy(c, h).start()

    eye = (
        lax.broadcasted_iota(jnp.int32, (per, per), 0)
        == lax.broadcasted_iota(jnp.int32, (per, per), 1)
    ).astype(F32).astype(BF16)
    mine = pl.ds(pl.multiple_of(me * per, per), per)
    for c in range(chunks):
        block = lax.dot_general(
            eye, dens[c * width:(c + 1) * width, :], NT, preferred_element_type=F32
        )
        x_buf[c, core, mine, :] = block.astype(BF16)

    def ring_copy(c, slot, origin, target):
        ref = x_buf.at[c, core, pl.ds(pl.multiple_of(origin * per, per), per), :]
        return pltpu.make_async_remote_copy(
            src_ref=ref, dst_ref=ref, send_sem=ring_send.at[c, slot],
            recv_sem=ring_recv.at[c, slot], device_id={"freq": target}, device_id_type=MESH,
        )

    def pair_copy(c, slot, origin, side):
        ref = x_buf.at[c, side, pl.ds(pl.multiple_of(origin * per, per), per), :]
        return pltpu.make_async_remote_copy(
            src_ref=ref, dst_ref=ref, send_sem=pair_send.at[c, slot],
            recv_sem=pair_recv.at[c, slot], device_id={"gvec": peer}, device_id_type=MESH,
        )

    def reach(c):
        ahead = mid if c % 2 == 0 else mid - 1
        return ahead, n - 1 - ahead

    pl.semaphore_wait(barrier, 3)
    for c in range(chunks):
        ring_copy(c, 0, me, right).start()
        ring_copy(c, mid, me, left).start()
    for c in range(chunks):
        pair_copy(c, 0, me, core).start()

    one_hot = (
        lax.broadcasted_iota(jnp.int32, (pairs, pairs), 0) == order[...]
    ).astype(F32)
    perm[...] = one_hot.T.astype(BF16)

    def take(c, d):
        ahead, behind = reach(c)
        if d <= ahead:
            origin = index_at((place + n - d) % n)
            ring_copy(c, d - 1, origin, right).wait_recv()
            if d < ahead:
                ring_copy(c, d, origin, right).start()
            pair_copy(c, d, origin, core).start()
        if d <= behind:
            origin = index_at((place + d) % n)
            ring_copy(c, mid + d - 1, origin, left).wait_recv()
            if d < behind:
                ring_copy(c, mid + d, origin, left).start()
            pair_copy(c, mid + d, origin, core).start()

    def from_peer(c):
        ahead, behind = reach(c)
        pair_copy(c, 0, me, peer).wait_recv()
        for d in range(1, ahead + 1):
            pair_copy(c, d, index_at((place + n - d) % n), peer).wait_recv()
        for d in range(1, behind + 1):
            pair_copy(c, mid + d, index_at((place + d) % n), peer).wait_recv()

    tile = rows // 3 if rows % 48 == 0 else rows

    def multiply(c):
        for h in range(2):
            w_copy(c, h).wait()
            e_buf[h, :, c * width:(c + 1) * width] = jnp.dot(
                perm[...], x_buf[c, h], preferred_element_type=F32
            ).astype(BF16)

        def step(t, _):
            at = pl.ds(pl.multiple_of(t * tile, tile), tile)
            total = sum(
                lax.dot_general(
                    w_buf[c, h, at, :], e_buf[h, :, c * width:(c + 1) * width], NT,
                    preferred_element_type=F32,
                )
                for h in range(2)
            )
            if c > 0:
                total = total + acc[at, :]
            if c < chunks - 1:
                acc[at, :] = total
            else:
                total = total.astype(BF16)
                p_buf[0, at, :] = total[:, :half]
                p_buf[1, at, :] = total[:, half:]
            return 0

        lax.fori_loop(0, rows // tile, step, 0)

    for d in range(1, mid):
        for c in range(chunks):
            take(c, d)
    for c in range(chunks):
        take(c, mid)
    for c in range(chunks):
        from_peer(c)
        multiply(c)

    def half_copy(i):
        return pltpu.make_async_remote_copy(
            src_ref=k_send.at[i], dst_ref=k_peer.at[i], send_sem=half_send.at[i],
            recv_sem=half_recv.at[i], device_id={"gvec": peer}, device_id_type=MESH,
        )

    def out_copy(target, slot):
        return pltpu.make_async_remote_copy(
            src_ref=k_red.at[pl.ds(pl.multiple_of(target * per, per), per), :],
            dst_ref=rows_in.at[me], send_sem=out_send.at[slot], recv_sem=out_recv.at[me],
            device_id={"freq": target}, device_id_type=MESH,
        )

    near = me // mid
    blocks = (1 - near, near)
    local = me % mid

    for i, b in enumerate(blocks):
        at = pl.ds(pl.multiple_of(b * half, half), half)
        k_send[i] = jnp.dot(e_buf[core, at, :], p_buf[peer], preferred_element_type=F32)
        half_copy(i).start()
    for i, b in enumerate(blocks):
        at = pl.ds(pl.multiple_of(b * half, half), half)
        k_own[i] = jnp.dot(e_buf[core, at, :], p_buf[core], preferred_element_type=F32)
    targets = []
    for i, b in enumerate(blocks):
        at = pl.ds(pl.multiple_of(b * half, half), half)
        half_copy(i).wait_recv()
        k_red[at, :] = (k_own[i] + k_peer[i]).astype(BF16)
        for t in range(i, mid):
            target = b * mid + (local + t) % mid
            out_copy(target, len(targets)).start()
            targets.append(target)
    rows_in[me] = k_red[mine, :]

    for t in range(1, n):
        source = (me + t) % n
        pltpu.make_async_remote_copy(
            src_ref=rows_in.at[source], dst_ref=rows_in.at[source],
            send_sem=out_send.at[0], recv_sem=out_recv.at[source],
            device_id={"freq": source}, device_id_type=MESH,
        ).wait_recv()
    for o in range(out.shape[0]):
        out[o] = sum(
            quad_table[quad_index[o, f]] * rows_in[f].astype(F32) for f in range(n)
        )

    for c in range(chunks):
        ahead, behind = reach(c)
        for d in range(ahead):
            ring_copy(c, d, me, right).wait_send()
        for d in range(behind):
            ring_copy(c, mid + d, me, left).wait_send()
        pair_copy(c, 0, me, core).wait_send()
        for d in range(1, ahead + 1):
            pair_copy(c, d, me, core).wait_send()
        for d in range(1, behind + 1):
            pair_copy(c, mid + d, me, core).wait_send()
    for i in range(2):
        half_copy(i).wait_send()
    for slot, target in enumerate(targets):
        out_copy(target, slot).wait_send()


def body(n, screened, densities, pair_order, quad_index, quad_table):
    rows, per = densities.shape
    pairs = n * per
    half = pairs // 2
    chunks = next(c for c in (4, 3, 2, 1) if rows % (c * 128) == 0 or c == 1)
    width = rows // chunks
    energies = quad_index.shape[0]
    slots = n + 1
    dma = pltpu.SemaphoreType.DMA
    vmem = pl.BlockSpec(memory_space=pltpu.VMEM)
    smem = pl.BlockSpec(memory_space=pltpu.SMEM)
    return pl.pallas_call(
        functools.partial(kernel, n, chunks),
        out_shape=jax.ShapeDtypeStruct((energies, per, half), F32),
        in_specs=[pl.BlockSpec(memory_space=pl.ANY), vmem, vmem, smem, smem],
        out_specs=vmem,
        scratch_shapes=[
            pltpu.VMEM((chunks, 2, rows, width), BF16),
            pltpu.VMEM((chunks, 2, pairs, width), BF16),
            pltpu.VMEM((2, pairs, rows), BF16),
            pltpu.VMEM((rows, pairs), F32),
            pltpu.VMEM((2, rows, half), BF16),
            pltpu.VMEM((pairs, pairs), BF16),
            pltpu.VMEM((2, half, half), F32),
            pltpu.VMEM((2, half, half), F32),
            pltpu.VMEM((2, half, half), F32),
            pltpu.VMEM((pairs, half), BF16),
            pltpu.VMEM((n, per, half), BF16),
            dma((chunks, 2)),
            dma((chunks, slots)), dma((chunks, slots)),
            dma((chunks, slots)), dma((chunks, slots)),
            dma((2,)), dma((2,)), dma((n,)), dma((n,)),
        ],
        compiler_params=pltpu.CompilerParams(
            collective_id=0, has_side_effects=True, vmem_limit_bytes=60 * 1024 * 1024
        ),
    )(screened, densities, pair_order[None, :], quad_index, quad_table)


def solution(mesh):
    placed = (P(("groups", "freq"), "gvec", None), P(("groups", "gvec"), "freq"), P(), P(), P())
    return jax.shard_map(
        functools.partial(body, mesh.shape["freq"]), mesh=mesh, in_specs=placed,
        out_specs=P("groups", "freq", "gvec"), check_vma=False,
    )
```

```python
import functools

import jax
import jax.numpy as jnp
from jax import lax
from jax.experimental import pallas as pl
from jax.experimental.pallas import tpu as pltpu
from jax.sharding import PartitionSpec as P

MESH = pl.DeviceIdType.MESH
F32 = jnp.float32
BF16 = jnp.bfloat16
NT = (((1,), (1,)), ((), ()))


def kernel(
    n, chunks, screened, dens, order, quad_index, quad_table, out,
    w_buf, x_buf, e_buf, acc, pa_buf, p_buf, perm, order_rows, k_send, k_peer, k_own, k_red, rows_in,
    own_sem, w_sem, ring_send, ring_recv, pair_send, pair_recv, half_send, half_recv, out_send, out_recv,
):
    per, rows = dens.shape
    pairs = n * per
    half = pairs // 2
    mid = n // 2
    width = rows // chunks
    me = lax.axis_index("freq")
    core = lax.axis_index("gvec")
    peer = 1 - core

    def index_at(position):
        fold = position // mid
        return (1 - fold) * (2 * position) + fold * (2 * (n - 1 - position) + 1)

    odd = me % 2
    place = (1 - odd) * (me // 2) + odd * (n - 1 - me // 2)
    right = index_at((place + 1) % n)
    left = index_at((place + n - 1) % n)

    barrier = pltpu.get_barrier_semaphore()
    pl.semaphore_signal(barrier, inc=1, device_id={"freq": left}, device_id_type=MESH)
    pl.semaphore_signal(barrier, inc=1, device_id={"freq": right}, device_id_type=MESH)
    pl.semaphore_signal(barrier, inc=1, device_id={"gvec": peer}, device_id_type=MESH)

    def w_copy(c, h):
        columns = pl.ds(h * rows + c * width, width)
        return pltpu.make_async_copy(
            screened.at[0, :, columns], w_buf.at[c, h], w_sem.at[c, h]
        )

    mine = pl.ds(pl.multiple_of(me * per, per), per)

    def own_copy(c):
        return pltpu.make_async_copy(
            dens.at[:, pl.ds(c * width, width)], x_buf.at[c, core, 0:per, :], own_sem.at[c]
        )

    for c in range(chunks):
        own_copy(c).start()

    def spot(d, side):
        return n - 1 if d == mid else max(0, 2 * d - 1 + side)

    def ring_copy(c, d, side, target):
        return pltpu.make_async_remote_copy(
            src_ref=x_buf.at[c, core, pl.ds(spot(d, side) * per, per), :],
            dst_ref=x_buf.at[c, core, pl.ds(spot(d + 1, side) * per, per), :],
            send_sem=ring_send.at[c, side * mid + d], recv_sem=ring_recv.at[c, side * mid + d],
            device_id={"freq": target}, device_id_type=MESH,
        )

    def pair_copy(c, at, core_from):
        ref = x_buf.at[c, core_from, pl.ds(at * per, per), :]
        return pltpu.make_async_remote_copy(
            src_ref=ref, dst_ref=ref, send_sem=pair_send.at[c, at],
            recv_sem=pair_recv.at[c, at], device_id={"gvec": peer}, device_id_type=MESH,
        )

    def reach(c):
        ahead = mid if c % 2 == 0 else mid - 1
        return ahead, n - 1 - ahead

    for c in range(chunks):
        own_copy(c).wait()
    pl.semaphore_wait(barrier, 3)
    for c in range(chunks):
        ring_copy(c, 0, 0, right).start()
        ring_copy(c, 0, 1, left).start()
    for c in range(chunks):
        pair_copy(c, 0, core).start()
    for c in range(chunks):
        for h in range(2):
            w_copy(c, h).start()

    for at in range(n):
        d, side = (at + 1) // 2, 1 - at % 2
        origin = index_at((place + (d if side else n - d)) % n)
        pair = lax.broadcasted_iota(jnp.int32, (per, pairs), 0) + origin * per
        one_hot = (pair == order[...]).astype(F32)
        order_rows[at * per:(at + 1) * per, :] = one_hot.astype(BF16)
    perm[...] = order_rows[...].astype(F32).T.astype(BF16)

    def take(c, d):
        for side, last, target in zip((0, 1), reach(c), (right, left)):
            if d <= last:
                ring_copy(c, d - 1, side, target).wait_recv()
                if d < last:
                    ring_copy(c, d, side, target).start()
                pair_copy(c, spot(d, side), core).start()

    tile = rows // 2 if rows % 32 == 0 else rows

    def multiply(c, g):
        for at in range(g * mid, (g + 1) * mid):
            pair_copy(c, at, peer).wait_recv()
        if g == 0:
            for h in range(2):
                w_copy(c, h).wait()
        members = slice(g * half, (g + 1) * half)

        def step(t, _):
            at = pl.ds(pl.multiple_of(t * tile, tile), tile)
            total = sum(
                lax.dot_general(
                    w_buf[c, h, at, :], x_buf[c, h, members, :], NT,
                    preferred_element_type=F32,
                )
                for h in range(2)
            )
            if c > 0:
                total = total + acc[g, at, :]
            if c < chunks - 1:
                acc[g, at, :] = total
                return 0
            total = total.astype(BF16)
            for h in range(2):
                part = jnp.dot(
                    total, order_rows[members, h * half:(h + 1) * half],
                    preferred_element_type=F32,
                )
                if g == 0:
                    pa_buf[h, at, :] = part.astype(BF16)
                else:
                    p_buf[h, at, :] = (part + pa_buf[h, at, :].astype(F32)).astype(BF16)
            return 0

        lax.fori_loop(0, rows // tile, step, 0)

    def order_own(c):
        e_buf[:, c * width:(c + 1) * width] = jnp.dot(
            perm[...], x_buf[c, core], preferred_element_type=F32
        ).astype(BF16)

    for d in range(1, mid // 2 + 1):
        for c in range(chunks):
            take(c, d)
    for c in range(chunks):
        multiply(c, 0)
        for d in range(mid // 2 + 1, mid):
            take(c, d)
    for c in range(chunks):
        take(c, mid)
    for c in range(chunks):
        order_own(c)
        multiply(c, 1)

    def half_copy(i):
        return pltpu.make_async_remote_copy(
            src_ref=k_send.at[i], dst_ref=k_peer.at[i], send_sem=half_send.at[i],
            recv_sem=half_recv.at[i], device_id={"gvec": peer}, device_id_type=MESH,
        )

    def out_copy(target, slot):
        return pltpu.make_async_remote_copy(
            src_ref=k_red.at[pl.ds(pl.multiple_of(target * per, per), per), :],
            dst_ref=rows_in.at[me], send_sem=out_send.at[slot], recv_sem=out_recv.at[me],
            device_id={"freq": target}, device_id_type=MESH,
        )

    near = me // mid
    blocks = (1 - near, near)
    local = me % mid

    for i, b in enumerate(blocks):
        at = pl.ds(pl.multiple_of(b * half, half), half)
        k_send[i] = jnp.dot(e_buf[at, :], p_buf[peer], preferred_element_type=F32)
        half_copy(i).start()
    for i, b in enumerate(blocks):
        at = pl.ds(pl.multiple_of(b * half, half), half)
        k_own[i] = jnp.dot(e_buf[at, :], p_buf[core], preferred_element_type=F32)
    targets = []
    for i, b in enumerate(blocks):
        at = pl.ds(pl.multiple_of(b * half, half), half)
        half_copy(i).wait_recv()
        k_red[at, :] = (k_own[i] + k_peer[i]).astype(BF16)
        for t in range(i, mid):
            target = b * mid + (local + t) % mid
            out_copy(target, len(targets)).start()
            targets.append(target)
    rows_in[me] = k_red[mine, :]

    for t in range(1, n):
        source = (me + t) % n
        pltpu.make_async_remote_copy(
            src_ref=rows_in.at[source], dst_ref=rows_in.at[source],
            send_sem=out_send.at[0], recv_sem=out_recv.at[source],
            device_id={"freq": source}, device_id_type=MESH,
        ).wait_recv()
    for o in range(out.shape[0]):
        out[o] = sum(
            quad_table[quad_index[o, f]] * rows_in[f].astype(F32) for f in range(n)
        )

    for c in range(chunks):
        for side, last, target in zip((0, 1), reach(c), (right, left)):
            for d in range(last):
                ring_copy(c, d, side, target).wait_send()
        for at in range(n):
            pair_copy(c, at, core).wait_send()
    for i in range(2):
        half_copy(i).wait_send()
    for slot, target in enumerate(targets):
        out_copy(target, slot).wait_send()


def body(n, screened, densities, pair_order, quad_index, quad_table):
    rows, per = densities.shape
    pairs = n * per
    half = pairs // 2
    chunks = next(c for c in (4, 3, 2, 1) if rows % (c * 128) == 0 or c == 1)
    width = rows // chunks
    energies = quad_index.shape[0]
    dma = pltpu.SemaphoreType.DMA
    hbm = pl.BlockSpec(memory_space=pl.ANY)
    vmem = pl.BlockSpec(memory_space=pltpu.VMEM)
    smem = pl.BlockSpec(memory_space=pltpu.SMEM)
    return pl.pallas_call(
        functools.partial(kernel, n, chunks),
        out_shape=jax.ShapeDtypeStruct((energies, per, half), F32),
        in_specs=[hbm, hbm, vmem, smem, smem],
        out_specs=vmem,
        scratch_shapes=[
            pltpu.VMEM((chunks, 2, rows, width), BF16),
            pltpu.VMEM((chunks, 2, pairs, width), BF16),
            pltpu.VMEM((pairs, rows), BF16),
            pltpu.VMEM((2, rows, half), F32),
            pltpu.VMEM((2, rows, half), BF16),
            pltpu.VMEM((2, rows, half), BF16),
            pltpu.VMEM((pairs, pairs), BF16),
            pltpu.VMEM((pairs, pairs), BF16),
            pltpu.VMEM((2, half, half), F32),
            pltpu.VMEM((2, half, half), F32),
            pltpu.VMEM((2, half, half), F32),
            pltpu.VMEM((pairs, half), BF16),
            pltpu.VMEM((n, per, half), BF16),
            dma((chunks,)), dma((chunks, 2)),
            dma((chunks, n)), dma((chunks, n)),
            dma((chunks, n)), dma((chunks, n)),
            dma((2,)), dma((2,)), dma((n,)), dma((n,)),
        ],
        compiler_params=pltpu.CompilerParams(
            collective_id=0, has_side_effects=True, vmem_limit_bytes=60 * 1024 * 1024
        ),
    )(screened, densities.T, pair_order[None, :], quad_index, quad_table)


def solution(mesh):
    placed = (P(("groups", "freq"), "gvec", None), P(("groups", "gvec"), "freq"), P(), P(), P())
    return jax.shard_map(
        functools.partial(body, mesh.shape["freq"]), mesh=mesh, in_specs=placed,
        out_specs=P("groups", "freq", "gvec"), check_vma=False,
    )
```
